32 devices in a mesh: tm: 4 (over y, x), space: 8 (over z, core).
Axes of the slice: x: 2, y: 2, z: 4, core: 2. Of those that a mesh axis runs over, the one named last changes fastest.
Arguments:
- residual: float32 [64, 64, 8, 128], P('tm', 'space'), may hold values from -24 to 24
- capacity: float32 [64, 8, 128], P('space'), may hold values from 0.25 to 4
Outputs:
- preconditioned: float32 [64, 64, 8, 128], P('tm', 'space')
The draws below stay inside these ranges and needn't reach their ends.
All inputs are finite; a program needn't handle non-finite values.
Results may differ from the reference program's by a relative error of at most 0.0003.
Values sent between devices are 32-bit elements; how exact they have to be, the bound alone decides.
A program may use at most 64 MiB of HBM per device.

```python
import math
import jax
import jax.numpy as jnp
from jax import lax

NY = 8
NZ = 128
TSTEPS = 64
GRID_DEPTH = 4
SMOOTH = 2
COARSE_SWEEPS = 6
NX = 64


def draw_residual(key, part):
    extents = (TSTEPS, NX, NY, NZ)
    return jnp.clip(4.0 * jax.random.normal(jax.random.fold_in(key, 11), extents, jnp.float32), -24.0, 24.0)


def levels(stream_key, shape, shards, smallest, high):
    loudness = 1.0
    for dim, parts in shards:
        steps = jax.random.uniform(jax.random.fold_in(jax.random.fold_in(stream_key, 6), dim), (parts,), jnp.float32, smallest / len(shards), high / len(shards))
        loudness = loudness * jnp.repeat(jnp.exp(steps), shape[dim] // parts).reshape((-1,) + (1,) * (len(shape) - 1 - dim))
    return loudness


def setup_inputs(seed: int = 0) -> dict:
    arg_keys = jax.random.split(jax.random.key(seed), 3)
    return {
        "residual": draw_residual(jax.random.fold_in(arg_keys[2], 71), 0),
        "capacity": jnp.clip(jnp.exp(math.log(4.0) - 2.7725887 * jax.random.uniform(arg_keys[1], (NX, NY, NZ), jnp.float32) ** levels(arg_keys[1], (NX, NY, NZ), ((0, 8),), -0.2, 0.2)), 0.25, 4.0),
    }


ALPHA_CORNER = 0.01
STEP_SIZE = 0.5
DIFFUSE = 2.0
ADVECT = (0.2, -0.15, 0.1)
OMEGA = 0.7
HIGHEST = lax.Precision.HIGHEST


def level_coefficients(per_level_values):
    spread = DIFFUSE / 4.0 ** per_level_values
    drifts = tuple(component / 2.0 ** per_level_values for component in ADVECT)
    return spread, drifts


def pad_second(volume, position):
    widths = [(0, 0)] * volume.ndim
    widths[position] = (1, 1)
    return jnp.pad(volume, widths)


def apply_operator(padded, current_capacity, spectral_shifts, per_level_values):
    spread, drifts = level_coefficients(per_level_values)
    centre = padded[:, :, 1:-1]
    upper_first = padded[:, :, 2:]
    lower_first = padded[:, :, :-2]
    wide_second = pad_second(centre, 3)
    upper_second = wide_second[:, :, :, 2:]
    lower_second = wide_second[:, :, :, :-2]
    wide_third = pad_second(centre, 4)
    upper_third = wide_third[:, :, :, :, 2:]
    lower_third = wide_third[:, :, :, :, :-2]
    stencil = spread * (6.0 * centre - upper_first - lower_first - upper_second - lower_second - upper_third - lower_third)
    stencil = stencil + drifts[0] * (upper_first - lower_first) + drifts[1] * (upper_second - lower_second) + drifts[2] * (upper_third - lower_third)
    first_shift, second_shift, third_shift = spectral_shifts
    real_part = centre[0]
    imag_part = centre[1]
    shifted = jnp.stack([current_capacity * (first_shift * real_part - second_shift * imag_part), current_capacity * (second_shift * real_part + third_shift * imag_part)])
    return stencil + shifted


def inverse_diagonal(current_capacity, spectral_shifts, per_level_values):
    spread, drifts = level_coefficients(per_level_values)
    first_shift, second_shift, third_shift = spectral_shifts
    top_left = current_capacity * first_shift + 6.0 * spread
    coupling = current_capacity * second_shift
    bottom_right = current_capacity * third_shift + 6.0 * spread
    determinant = top_left * bottom_right + coupling * coupling
    return bottom_right / determinant, coupling / determinant, top_left / determinant


def damped_update(residual_now, inverse):
    diagonal_a, diagonal_b, diagonal_c = inverse
    return OMEGA * jnp.stack([diagonal_a * residual_now[0] + diagonal_b * residual_now[1], diagonal_c * residual_now[1] - diagonal_b * residual_now[0]])


def restrict_to_coarse(volume):
    leading = volume.shape[:-3]
    first_extent, second_extent, third_extent = volume.shape[-3:]
    blocks = volume.reshape(leading + (first_extent // 2, 2, second_extent // 2, 2, third_extent // 2, 2))
    lead_count = len(leading)
    return jnp.mean(blocks, axis=(lead_count + 1, lead_count + 3, lead_count + 5))


def prolong_cells(volume):
    leading = volume.shape[:-3]
    first_extent, second_extent, third_extent = volume.shape[-3:]
    expanded = jnp.broadcast_to(volume[..., :, None, :, None, :, None], leading + (first_extent, 2, second_extent, 2, third_extent, 2))
    return expanded.reshape(leading + (2 * first_extent, 2 * second_extent, 2 * third_extent))


def shift_values(frequency, length):
    ratio_step = ALPHA_CORNER ** (1.0 / length)
    phases = (2.0 * math.pi / length) * frequency.astype(jnp.float32)
    first_shift = (1.0 - ratio_step * jnp.cos(phases)) / STEP_SIZE
    second_shift = ratio_step * jnp.sin(phases) / STEP_SIZE
    return tuple(column.reshape(-1, 1, 1, 1) for column in (first_shift, second_shift, first_shift))


def multigrid_cycle(per_level_values, forcing_term, capacity_fields, spectral_shifts):
    current_capacity = capacity_fields[per_level_values]
    inverse = inverse_diagonal(current_capacity, spectral_shifts, per_level_values)
    coarsest = per_level_values == GRID_DEPTH - 1
    current = damped_update(forcing_term, inverse)
    for repeat in range((COARSE_SWEEPS if coarsest else SMOOTH) - 1):
        current = current + damped_update(forcing_term - apply_operator(pad_second(current, 2), current_capacity, spectral_shifts, per_level_values), inverse)
    if coarsest:
        return current
    coarse_right_hand = restrict_to_coarse(forcing_term - apply_operator(pad_second(current, 2), current_capacity, spectral_shifts, per_level_values))
    coarse_solution = multigrid_cycle(per_level_values + 1, coarse_right_hand, capacity_fields, spectral_shifts)
    current = current + prolong_cells(coarse_solution)
    for repeat in range(SMOOTH):
        current = current + damped_update(forcing_term - apply_operator(pad_second(current, 2), current_capacity, spectral_shifts, per_level_values), inverse)
    return current


def reference(residual, capacity):
    length = residual.shape[0]
    ratio_step = ALPHA_CORNER ** (1.0 / length)
    moments = jnp.arange(length, dtype=jnp.float32)
    weights = jnp.power(ratio_step, moments)
    scaled = residual * weights[:, None, None, None]
    capacity_fields = [capacity]
    for per_level_values in range(1, GRID_DEPTH):
        capacity_fields.append(restrict_to_coarse(capacity_fields[-1]))
    integers = jnp.arange(length, dtype=jnp.int32)

    def one_frequency(summed, frequency):
        phases = (2.0 * math.pi / length) * ((integers * frequency) % length).astype(jnp.float32)
        cosines = jnp.cos(phases)
        sines = jnp.sin(phases)
        real_part = jnp.tensordot(cosines, scaled, axes=1, precision=HIGHEST)
        imag_part = -jnp.tensordot(sines, scaled, axes=1, precision=HIGHEST)
        forcing_term = jnp.stack([real_part, imag_part])[:, None]
        spectral_shifts = shift_values(frequency[None], length)
        solution_field = multigrid_cycle(0, forcing_term, capacity_fields, spectral_shifts)[:, 0]
        summed = summed + cosines[:, None, None, None] * solution_field[0] - sines[:, None, None, None] * solution_field[1]
        return summed, None

    summed, unused = lax.scan(one_frequency, jnp.zeros(residual.shape, jnp.float32), integers)
    return summed / length / weights[:, None, None, None]
```

```python
import functools
import math

import jax
import jax.numpy as jnp
import numpy as np
from jax import lax
from jax.experimental import pallas as pl
from jax.experimental.pallas import tpu as pltpu
from jax.sharding import PartitionSpec as P

GRID_DEPTH = 4
SMOOTH = 2
COARSE_SWEEPS = 6


ALPHA_CORNER = 0.01
STEP_SIZE = 0.5
DIFFUSE = 2.0
ADVECT = (0.2, -0.15, 0.1)
OMEGA = 0.7
HIGHEST = lax.Precision.HIGHEST


def extended(array, sides, width):
    for axis, dim in sides:
        peers, length = (lax.axis_size(axis), array.shape[dim])
        up = [(i, (i + 1) % peers) for i in range(peers - 1)]
        down = [(j, i) for i, j in up]
        last = lax.slice_in_dim(array, length - width, length, axis=dim)
        initial = lax.slice_in_dim(array, 0, width, axis=dim)
        before = lax.ppermute(last, axis, up)
        after = lax.ppermute(initial, axis, down)
        array = jnp.concatenate([before, array, after], axis=dim)
    return array


def level_coefficients(per_level_values):
    spread = DIFFUSE / 4.0**per_level_values
    drifts = tuple((component / 2.0**per_level_values for component in ADVECT))
    return (spread, drifts)


def pad_second(volume, position):
    widths = [(0, 0)] * volume.ndim
    widths[position] = (1, 1)
    return jnp.pad(volume, widths)


def apply_operator(padded, current_capacity, spectral_shifts, per_level_values):
    spread, drifts = level_coefficients(per_level_values)
    centre = padded[:, :, 1:-1]
    upper_first = padded[:, :, 2:]
    lower_first = padded[:, :, :-2]
    wide_second = pad_second(centre, 3)
    upper_second = wide_second[:, :, :, 2:]
    lower_second = wide_second[:, :, :, :-2]
    wide_third = pad_second(centre, 4)
    upper_third = wide_third[:, :, :, :, 2:]
    lower_third = wide_third[:, :, :, :, :-2]
    stencil = spread * (
        6.0 * centre
        - upper_first
        - lower_first
        - upper_second
        - lower_second
        - upper_third
        - lower_third
    )
    stencil = (
        stencil
        + drifts[0] * (upper_first - lower_first)
        + drifts[1] * (upper_second - lower_second)
        + drifts[2] * (upper_third - lower_third)
    )
    first_shift, second_shift, third_shift = spectral_shifts
    real_part = centre[0]
    imag_part = centre[1]
    shifted = jnp.stack(
        [
            current_capacity * (first_shift * real_part - second_shift * imag_part),
            current_capacity * (second_shift * real_part + third_shift * imag_part),
        ]
    )
    return stencil + shifted


def inverse_diagonal(current_capacity, spectral_shifts, per_level_values):
    spread, drifts = level_coefficients(per_level_values)
    first_shift, second_shift, third_shift = spectral_shifts
    top_left = current_capacity * first_shift + 6.0 * spread
    coupling = current_capacity * second_shift
    bottom_right = current_capacity * third_shift + 6.0 * spread
    determinant = top_left * bottom_right + coupling * coupling
    return (bottom_right / determinant, coupling / determinant, top_left / determinant)


def damped_update(residual_now, inverse):
    diagonal_a, diagonal_b, diagonal_c = inverse
    return OMEGA * jnp.stack(
        [
            diagonal_a * residual_now[0] + diagonal_b * residual_now[1],
            diagonal_c * residual_now[1] - diagonal_b * residual_now[0],
        ]
    )


def restrict_to_coarse(volume):
    leading = volume.shape[:-3]
    first_extent, second_extent, third_extent = volume.shape[-3:]
    blocks = volume.reshape(
        leading + (first_extent // 2, 2, second_extent // 2, 2, third_extent // 2, 2)
    )
    lead_count = len(leading)
    return jnp.mean(blocks, axis=(lead_count + 1, lead_count + 3, lead_count + 5))


def prolong_cells(volume):
    leading = volume.shape[:-3]
    first_extent, second_extent, third_extent = volume.shape[-3:]
    expanded = jnp.broadcast_to(
        volume[..., :, None, :, None, :, None],
        leading + (first_extent, 2, second_extent, 2, third_extent, 2),
    )
    return expanded.reshape(leading + (2 * first_extent, 2 * second_extent, 2 * third_extent))


def shift_values(frequency, length):
    ratio_step = ALPHA_CORNER ** (1.0 / length)
    phases = 2.0 * math.pi / length * frequency.astype(jnp.float32)
    first_shift = (1.0 - ratio_step * jnp.cos(phases)) / STEP_SIZE
    second_shift = ratio_step * jnp.sin(phases) / STEP_SIZE
    leading = frequency == 0
    second_shift = jnp.where(leading, 0.0, second_shift)
    third_shift = jnp.where(leading, (1.0 + ratio_step) / STEP_SIZE, first_shift)
    return tuple(
        (column.reshape(-1, 1, 1, 1) for column in (first_shift, second_shift, third_shift))
    )


def phase_grid(row_count, length):
    integers = (
        jnp.arange(row_count, dtype=jnp.int32)[:, None]
        * jnp.arange(length, dtype=jnp.int32)[None, :]
        % length
    )
    return 2.0 * math.pi / length * integers.astype(jnp.float32)


def pad_faces(volume):
    return extended(volume, (("space", 2),), 1)


def multigrid_cycle(
    per_level_values,
    forcing_term,
    capacity_fields,
    spectral_shifts,
    shared_values,
    assemble_level,
    assemble_parts,
):
    current_capacity = capacity_fields[per_level_values]
    inverse = inverse_diagonal(current_capacity, spectral_shifts, per_level_values)
    coarsest = per_level_values == GRID_DEPTH - 1
    current = damped_update(forcing_term, inverse)
    for repeat in range((COARSE_SWEEPS if coarsest else SMOOTH) - 1):
        current = current + damped_update(
            forcing_term
            - apply_operator(
                pad_faces(current), current_capacity, spectral_shifts, per_level_values
            ),
            inverse,
        )
    if coarsest:
        return current
    coarse_right_hand = restrict_to_coarse(
        forcing_term
        - apply_operator(pad_faces(current), current_capacity, spectral_shifts, per_level_values)
    )
    coarse_solution = multigrid_cycle(
        per_level_values + 1,
        coarse_right_hand,
        capacity_fields,
        spectral_shifts,
        shared_values,
        assemble_level,
        assemble_parts,
    )
    current = current + prolong_cells(coarse_solution)
    for repeat in range(SMOOTH):
        current = current + damped_update(
            forcing_term
            - apply_operator(
                pad_faces(current), current_capacity, spectral_shifts, per_level_values
            ),
            inverse,
        )
    return current


def on_device(residual, capacity):
    steps_here, thickness, extent_second, extent_third = residual.shape
    length = lax.axis_size("tm") * steps_here
    ratio_step = ALPHA_CORNER ** (1.0 / length)
    moments = (lax.axis_index("tm") * steps_here + jnp.arange(steps_here, dtype=jnp.int32)).astype(
        jnp.float32
    )
    scaled = (residual * jnp.power(ratio_step, moments)[:, None, None, None]).reshape(
        steps_here, -1
    )
    series = lax.all_to_all(scaled, "tm", split_axis=1, concat_axis=0, tiled=True)
    all_weights = jnp.power(ratio_step, jnp.arange(length, dtype=jnp.float32))
    alternate = 1.0 - 2.0 * (jnp.arange(length, dtype=jnp.int32) % 2).astype(jnp.float32)
    capacity_fields = [capacity]
    for per_level_values in range(1, GRID_DEPTH):
        capacity_fields.append(restrict_to_coarse(capacity_fields[-1]))
    halves = length // 2
    phases = phase_grid(halves, length)
    first_row = jnp.arange(halves, dtype=jnp.int32)[:, None] == 0
    forward = jnp.concatenate(
        [jnp.cos(phases), jnp.where(first_row, alternate[None, :], -jnp.sin(phases))], axis=0
    )
    spectrum = jnp.dot(forward, series, precision=HIGHEST).reshape(2, halves, -1)
    received = lax.all_to_all(spectrum, "tm", split_axis=1, concat_axis=2, tiled=True)
    slot_count = steps_here // 2
    frequency = lax.axis_index("tm") * slot_count + jnp.arange(slot_count, dtype=jnp.int32)
    spectral_shifts = shift_values(frequency, length)
    field_list = received.reshape(2, slot_count, thickness, extent_second, extent_third)
    solved_fields = multigrid_cycle(
        0, field_list, capacity_fields, spectral_shifts, False, GRID_DEPTH, None
    )
    flattened = solved_fields.reshape(2, slot_count, -1)
    returned = lax.all_to_all(flattened, "tm", split_axis=2, concat_axis=1, tiled=True)
    halves = length // 2
    phases = jnp.transpose(phase_grid(halves, length))
    first_column = jnp.arange(halves, dtype=jnp.int32)[None, :] == 0
    real_columns = jnp.where(first_column, 1.0, 2.0 * jnp.cos(phases)) / length
    imag_columns = jnp.where(first_column, alternate[:, None], -2.0 * jnp.sin(phases)) / length
    inverse_table = jnp.concatenate([real_columns, imag_columns], axis=1)
    values = jnp.dot(
        inverse_table,
        returned.reshape(returned.shape[0] * returned.shape[1], -1),
        precision=HIGHEST,
    )
    values = values / all_weights[:, None]
    result = lax.all_to_all(values, "tm", split_axis=0, concat_axis=1, tiled=True)
    return result.reshape(residual.shape)


MESH = pl.DeviceIdType.MESH


def real_transform(values):
    count = len(values)
    if count == 1:
        return [(values[0], None)]
    evens, odds = real_transform(values[0::2]), real_transform(values[1::2])
    half = count // 2
    if count == 2:
        return [(evens[0][0] + odds[0][0], None), (evens[0][0] - odds[0][0], None)]
    found = [None] * (half + 1)
    found[0] = (evens[0][0] + odds[0][0], None)
    found[half] = (evens[0][0] - odds[0][0], None)
    found[half // 2] = (evens[half // 2][0], -odds[half // 2][0])
    for k in range(1, half // 2):
        cosine, sine = math.cos(2 * math.pi * k / count), -math.sin(2 * math.pi * k / count)
        (er, ei), (or_, oi) = evens[k], odds[k]
        tr, ti = cosine * or_ - sine * oi, cosine * oi + sine * or_
        found[k] = (er + tr, ei + ti)
        found[half - k] = (er - tr, ti - ei)
    return found


def real_inverse(modes):
    half = len(modes) - 1
    if half == 0:
        return [modes[0][0]]
    count = 2 * half
    if half == 1:
        return [modes[0][0] + modes[1][0], modes[0][0] - modes[1][0]]
    evens, odds = [None] * (half // 2 + 1), [None] * (half // 2 + 1)
    evens[0] = (modes[0][0] + modes[half][0], None)
    odds[0] = (modes[0][0] - modes[half][0], None)
    middle = modes[half // 2]
    evens[half // 2] = (2.0 * middle[0], None)
    odds[half // 2] = (-2.0 * middle[1], None)
    for k in range(1, half // 2):
        cosine, sine = math.cos(2 * math.pi * k / count), math.sin(2 * math.pi * k / count)
        (ar, ai), (br, bi) = modes[k], modes[half - k]
        dr, di = ar - br, ai + bi
        evens[k] = (ar + br, ai - bi)
        odds[k] = (cosine * dr - sine * di, cosine * di + sine * dr)
    first, second = real_inverse(evens), real_inverse(odds)
    return [part for pair in zip(first, second) for part in pair]


def pair_sum(value, distance):
    for axis in (-2, -1):
        dim = value.ndim + axis
        extent = value.shape[dim]
        upper = pltpu.roll(value, extent - distance, dim)
        lower = pltpu.roll(value, distance, dim)
        place = lax.broadcasted_iota(jnp.int32, value.shape, dim)
        value = value + jnp.where((place // distance) % 2 == 0, upper, lower)
    return value


def block_mean(value, distance):
    shape = (value.shape[0] // 2, 2) + value.shape[1:]
    paired = value.reshape(shape)
    return 0.125 * pair_sum(paired[:, 0] + paired[:, 1], distance)


def neighbour_weights(level, shape):
    spread, drifts = level_coefficients(level)
    distance = 2**level
    along_first = (drifts[0] - spread, -drifts[0] - spread)
    masked = []
    for dim in (0, 1):
        place = lax.broadcasted_iota(jnp.int32, shape, dim)
        upper = jnp.where(place < shape[dim] - distance, drifts[dim + 1] - spread, 0.0)
        lower = jnp.where(place >= distance, -drifts[dim + 1] - spread, 0.0)
        masked.append((upper, lower))
    return along_first, masked, distance


def neighbours(wide, weights):
    along_first, masked, distance = weights
    centre = wide[1:-1]
    total = along_first[0] * wide[2:] + along_first[1] * wide[:-2]
    for dim in (0, 1):
        extent = centre.shape[dim + 1]
        if distance >= extent:
            continue
        upper, lower = masked[dim]
        total = total + upper[None] * pltpu.roll(centre, extent - distance, dim + 1)
        total = total + lower[None] * pltpu.roll(centre, distance, dim + 1)
    return total


def blocks_of(extent, largest, body):
    block = min(extent, largest)

    def step(i, carry):
        body(pl.multiple_of(i * block, block), block)
        return carry

    if extent == block:
        body(0, block)
    else:
        lax.fori_loop(0, extent // block, step, 0)


BLOCK = 4


def prepare_level(level, caps, inverses, shifts):
    spread, unused = level_coefficients(level)
    s1, s2, s3 = shifts

    def body(start, block):
        cap = caps[level][pl.ds(start, block)]
        top, coupling, bottom = cap * s1 + 6.0 * spread, cap * s2, cap * s3 + 6.0 * spread
        scale = OMEGA / (top * bottom + coupling * coupling)
        inverses[level][pl.ds(start, block), 0] = bottom * scale
        inverses[level][pl.ds(start, block), 1] = coupling * scale
        inverses[level][pl.ds(start, block), 2] = top * scale
        if level + 1 < GRID_DEPTH:
            half = block // 2
            caps[level + 1][pl.ds(start // 2, half)] = block_mean(cap, 2**level)

    blocks_of(caps[level].shape[0], BLOCK, body)


def smooth_first(forcing, target, inverse):
    def body(start, block):
        here = pl.ds(start, block)
        a, b, c = inverse[here, 0], inverse[here, 1], inverse[here, 2]
        re, im = forcing[here, 0], forcing[here, 1]
        there = pl.ds(start + 1, block)
        target[there, 0] = a * re + b * im
        target[there, 1] = c * im - b * re

    blocks_of(forcing.shape[0], BLOCK, body)


def smooth(forcing, source, target, inverse, weights, offset=1, coarse=None):
    def body(start, block):
        here = pl.ds(start, block)
        wide_re = source[pl.ds(start, block + 2), 0]
        wide_im = source[pl.ds(start, block + 2), 1]
        r0 = forcing[here, 0] - neighbours(wide_re, weights)
        r1 = forcing[here, 1] - neighbours(wide_im, weights)
        a, b, c = inverse[here, 0], inverse[here, 1], inverse[here, 2]
        there = pl.ds(start + offset, block)
        target[there, 0] = (1.0 - OMEGA) * wide_re[1:-1] + (a * r0 + b * r1)
        target[there, 1] = (1.0 - OMEGA) * wide_im[1:-1] + (c * r1 - b * r0)

    blocks_of(forcing.shape[0], BLOCK, body)


def restrict_residual(level, forcing, source, cap, shifts, weights, target):
    spread, unused = level_coefficients(level)
    s1, s2, s3 = shifts

    def body(start, block):
        here = pl.ds(start, block)
        wide_re = source[pl.ds(start, block + 2), 0]
        wide_im = source[pl.ds(start, block + 2), 1]
        re, im = wide_re[1:-1], wide_im[1:-1]
        field = cap[here]
        r0 = forcing[here, 0] - neighbours(wide_re, weights)
        r1 = forcing[here, 1] - neighbours(wide_im, weights)
        r0 = r0 - (6.0 * spread * re + field * (s1 * re - s2 * im))
        r1 = r1 - (6.0 * spread * im + field * (s2 * re + s3 * im))
        half = pl.ds(start // 2, block // 2)
        target[half, 0] = block_mean(r0, 2**level)
        target[half, 1] = block_mean(r1, 2**level)

    blocks_of(forcing.shape[0], BLOCK, body)


def add_coarse(target, coarse):
    def body(start, block):
        half = block // 2
        for part in (0, 1):
            extra = coarse[pl.ds(start // 2 + 1, half), part]
            spread = jnp.broadcast_to(extra[:, None], (half, 2) + extra.shape[1:])
            there = pl.ds(start + 1, block)
            target[there, part] = target[there, part] + spread.reshape((block,) + extra.shape[1:])

    blocks_of(target.shape[0] - 2, BLOCK, body)


def cycle(level, forcings, caps, inverses, firsts, seconds, shifts, result):
    forcing, inverse = forcings[level], inverses[level]
    here, other = firsts[level], seconds[level]
    weights = neighbour_weights(level, forcing.shape[-2:])
    coarsest = level == GRID_DEPTH - 1
    smooth_first(forcing, here, inverse)
    for repeat in range((COARSE_SWEEPS if coarsest else SMOOTH) - 1):
        smooth(forcing, here, other, inverse, weights)
        here, other = other, here
    if coarsest:
        return here
    restrict_residual(level, forcing, here, caps[level], shifts, weights, forcings[level + 1])
    coarse = cycle(level + 1, forcings, caps, inverses, firsts, seconds, shifts, None)
    add_coarse(here, coarse)
    for repeat in range(SMOOTH):
        last = repeat == SMOOTH - 1 and result is not None
        target = result if last else other
        smooth(forcing, here, target, inverse, weights, offset=0 if last else 1)
        here, other = target, here
    return here


def whole_kernel(groups, slabs, shift_ref, residual_ref, capacity_ref, out_ref, *scratch):
    (series, spectrum, returned, values, result) = scratch[:5]
    depth = GRID_DEPTH
    forcings = scratch[5 : 5 + depth]
    caps = scratch[5 + depth : 5 + 2 * depth]
    inverses = scratch[5 + 2 * depth : 5 + 3 * depth]
    firsts = scratch[5 + 3 * depth : 5 + 4 * depth]
    seconds = scratch[5 + 4 * depth : 5 + 5 * depth]
    send1, recv1, send2, recv2, send3, recv3, send4, recv4, own, sendc, recvc = scratch[
        5 + 5 * depth :
    ]
    steps, thick = residual_ref.shape[:2]
    planes = thick // groups
    length = groups * steps
    devices = groups * slabs
    ratio_step = ALPHA_CORNER ** (1.0 / length)
    mine, slab = lax.axis_index("tm"), lax.axis_index("space")
    me = mine * slabs + slab
    base = slab * thick + mine * planes

    def peer_of(k):
        peer = lax.rem(me + k, devices)
        return peer, peer // slabs, lax.rem(peer, slabs)

    barrier = pltpu.get_barrier_semaphore()

    def greet(k, carry):
        unused, to_tm, to_space = peer_of(k)
        pl.semaphore_signal(barrier, inc=1, device_id=(to_tm, to_space), device_id_type=MESH)
        return carry

    lax.fori_loop(1, devices, greet, 0)
    for level in range(depth):
        for buffer in (firsts[level], seconds[level]):
            empty = jnp.zeros(buffer.shape[1:], jnp.float32)
            buffer[0] = empty
            buffer[buffer.shape[0] - 1] = empty
    pl.semaphore_wait(barrier, devices - 1)

    first_sends = []
    for p in range(planes):
        for d in range(1, groups):
            to_tm = lax.rem(mine + d, groups)
            copy = pltpu.make_async_remote_copy(
                src_ref=residual_ref.at[:, to_tm * planes + p],
                dst_ref=series.at[p, pl.ds(mine * steps, steps)],
                send_sem=send1.at[p, d],
                recv_sem=recv1.at[p, d],
                device_id=(to_tm, slab),
                device_id_type=MESH,
            )
            copy.start()
            first_sends.append(copy)
    own_steps = []
    for p in range(planes):
        copy = pltpu.make_async_copy(
            residual_ref.at[:, mine * planes + p],
            series.at[p, pl.ds(mine * steps, steps)],
            own.at[p],
        )
        copy.start()
        own_steps.append(copy)

    own_slab = pl.ds(slab * thick, thick)
    caps[0][own_slab] = capacity_ref[...]
    cap_sends = []
    for d in range(1, slabs // 2):
        copy = pltpu.make_async_remote_copy(
            src_ref=capacity_ref,
            dst_ref=caps[0].at[own_slab],
            send_sem=sendc.at[d],
            recv_sem=recvc.at[d],
            device_id=(mine, lax.rem(slab + 2 * d, slabs)),
            device_id_type=MESH,
        )
        copy.start()
        cap_sends.append(copy)
    parity = lax.rem(slab, 2)
    partner = slab + 1 - 2 * parity

    def forward_cap(d):
        index = lax.rem(slab + slabs - 2 * d, slabs)
        rows = pl.ds(index * thick, thick)
        copy = pltpu.make_async_remote_copy(
            src_ref=capacity_ref if d == 0 else caps[0].at[rows],
            dst_ref=caps[0].at[rows],
            send_sem=sendc.at[slabs // 2 + d],
            recv_sem=recvc.at[slabs // 2 + d],
            device_id=(mine, partner),
            device_id_type=MESH,
        )
        copy.start()
        return copy

    cap_forwards = [forward_cap(0)]

    def spread_mode(k, p):
        peer, to_tm, to_space = peer_of(k)
        return pltpu.make_async_remote_copy(
            src_ref=spectrum.at[p, peer],
            dst_ref=forcings[0].at[base + p],
            send_sem=send2.at[p],
            recv_sem=recv2.at[p],
            device_id=(to_tm, to_space),
            device_id_type=MESH,
        )

    own_modes = []
    for p in range(planes):
        own_steps[p].wait()
        for d in range(1, groups):
            first_sends[p * (groups - 1) + d - 1].wait_recv()
        modes = real_transform([ratio_step**t * series[p, t] for t in range(length)])
        spectrum[p, 0, 0] = modes[0][0]
        spectrum[p, 0, 1] = modes[length // 2][0]
        for k in range(1, length // 2):
            spectrum[p, k, 0] = modes[k][0]
            spectrum[p, k, 1] = modes[k][1]

        def start_mode(k, carry):
            spread_mode(k, p).start()
            return carry

        lax.fori_loop(1, devices, start_mode, 0)
        copy = pltpu.make_async_copy(
            spectrum.at[p, me], forcings[0].at[base + p], own.at[planes + p]
        )
        copy.start()
        own_modes.append(copy)
        if p == 0:
            for d in range(1, slabs // 2):
                cap_sends[d - 1].wait_recv()
                cap_forwards.append(forward_cap(d))

    for copy in cap_forwards:
        copy.wait_recv()
    shifts = tuple(shift_ref[me, j] for j in range(3))
    for level in range(depth):
        prepare_level(level, caps, inverses, shifts)

    def all_but_one(array, semaphore):
        part = array.at[pl.ds(0, devices - 1)]
        return pltpu.make_async_copy(part, part, semaphore)

    for p in range(planes):
        own_modes[p].wait()
        all_but_one(forcings[0], recv2.at[p]).wait()

    cycle(0, forcings, caps, inverses, firsts, seconds, shifts, result)

    def send_back(k, p):
        peer, to_tm, to_space = peer_of(k)
        return pltpu.make_async_remote_copy(
            src_ref=result.at[to_space * thick + to_tm * planes + p],
            dst_ref=returned.at[p, me],
            send_sem=send3.at[p],
            recv_sem=recv3.at[p],
            device_id=(to_tm, to_space),
            device_id_type=MESH,
        )

    own_back = []
    for p in range(planes):

        def start_back(k, carry):
            send_back(k, p).start()
            return carry

        lax.fori_loop(1, devices, start_back, 0)
        copy = pltpu.make_async_copy(
            result.at[base + p], returned.at[p, me], own.at[2 * planes + p]
        )
        copy.start()
        own_back.append(copy)

    last_copies = []
    for p in range(planes):
        own_back[p].wait()
        all_but_one(returned.at[p], recv3.at[p]).wait()
        modes = [(returned[p, 0, 0], None)]
        modes += [(returned[p, k, 0], returned[p, k, 1]) for k in range(1, length // 2)]
        modes += [(returned[p, 0, 1], None)]
        for t, value in enumerate(real_inverse(modes)):
            values[p, t] = value * (ratio_step**-t / length)
        for d in range(1, groups):
            to_tm = lax.rem(mine + d, groups)
            copy = pltpu.make_async_remote_copy(
                src_ref=values.at[p, pl.ds(to_tm * steps, steps)],
                dst_ref=out_ref.at[:, mine * planes + p],
                send_sem=send4.at[p, d],
                recv_sem=recv4.at[p, d],
                device_id=(to_tm, slab),
                device_id_type=MESH,
            )
            copy.start()
            last_copies.append(copy)
        out_ref[:, mine * planes + p] = values[p, pl.ds(mine * steps, steps)]

    for copy in last_copies:
        copy.wait()
    for copy in first_sends + cap_sends + cap_forwards:
        copy.wait_send()
    for p in range(planes):
        all_but_one(spectrum.at[p], send2.at[p]).wait()
        all_but_one(result, send3.at[p]).wait()


def fused(groups, slabs, residual, capacity):
    steps, thick, second, third = residual.shape
    length, devices = groups * steps, groups * slabs
    planes, extent = thick // groups, slabs * thick
    tile = (second, third)
    ratio_step = ALPHA_CORNER ** (1.0 / length)
    angle = 2.0 * np.pi / length * np.arange(devices)
    table = np.stack(
        [
            (1.0 - ratio_step * np.cos(angle)) / STEP_SIZE,
            ratio_step * np.sin(angle) / STEP_SIZE,
            (1.0 - ratio_step * np.cos(angle)) / STEP_SIZE,
        ],
        axis=1,
    )
    table[0, 1], table[0, 2] = 0.0, (1.0 + ratio_step) / STEP_SIZE
    extents = [extent // 2**level for level in range(GRID_DEPTH)]
    vmem = lambda *shape: pltpu.VMEM(shape + tile, jnp.float32)
    sems = lambda *shape: pltpu.SemaphoreType.DMA(shape)
    scratch = [
        vmem(planes, length),
        vmem(planes, devices, 2),
        vmem(planes, devices, 2),
        vmem(planes, length),
        vmem(extent, 2),
        *[vmem(n, 2) for n in extents],
        *[vmem(n) for n in extents],
        *[vmem(n, 3) for n in extents],
        *[vmem(n + 2, 2) for n in extents],
        *[vmem(n + 2, 2) for n in extents],
        sems(planes, groups),
        sems(planes, groups),
        sems(planes),
        sems(planes),
        sems(planes),
        sems(planes),
        sems(planes, groups),
        sems(planes, groups),
        sems(3 * planes),
        sems(slabs),
        sems(slabs),
    ]
    return pl.pallas_call(
        functools.partial(whole_kernel, groups, slabs),
        out_shape=jax.ShapeDtypeStruct(residual.shape, jnp.float32),
        in_specs=[
            pl.BlockSpec(memory_space=pltpu.SMEM),
            pl.BlockSpec(memory_space=pltpu.VMEM),
            pl.BlockSpec(memory_space=pltpu.VMEM),
        ],
        out_specs=pl.BlockSpec(memory_space=pltpu.VMEM),
        scratch_shapes=scratch,
        compiler_params=pltpu.CompilerParams(
            collective_id=0, has_side_effects=True, vmem_limit_bytes=32 * 2**20
        ),
    )(jnp.asarray(table, jnp.float32), residual, capacity)


def fits_fused(groups, slabs, residual):
    steps, thick, second, third = residual.shape
    length = groups * steps
    power = length & (length - 1) == 0
    return (
        power
        and groups * slabs == length // 2
        and slabs % 2 == 0
        and thick % groups == 0
        and (slabs * thick) % (BLOCK * 2 ** (GRID_DEPTH - 1)) == 0
        and (second, third) == (8, 128)
    )


def either(residual, capacity):
    groups, slabs = lax.axis_size("tm"), lax.axis_size("space")
    if fits_fused(groups, slabs, residual):
        return fused(groups, slabs, residual, capacity)
    return on_device(residual, capacity)


def solution(mesh):
    return jax.shard_map(
        either,
        mesh=mesh,
        in_specs=(P("tm", "space", None, None), P("space", None, None)),
        out_specs=P("tm", "space", None, None),
        check_vma=False,
    )
```

```python
import functools
import math

import jax
import jax.numpy as jnp
import numpy as np
from jax import lax
from jax.experimental import pallas as pl
from jax.experimental.pallas import tpu as pltpu
from jax.sharding import PartitionSpec as P

GRID_DEPTH = 4
SMOOTH = 2
COARSE_SWEEPS = 6


ALPHA_CORNER = 0.01
STEP_SIZE = 0.5
DIFFUSE = 2.0
ADVECT = (0.2, -0.15, 0.1)
OMEGA = 0.7
HIGHEST = lax.Precision.HIGHEST


def extended(array, sides, width):
    for axis, dim in sides:
        peers, length = (lax.axis_size(axis), array.shape[dim])
        up = [(i, (i + 1) % peers) for i in range(peers - 1)]
        down = [(j, i) for i, j in up]
        last = lax.slice_in_dim(array, length - width, length, axis=dim)
        initial = lax.slice_in_dim(array, 0, width, axis=dim)
        before = lax.ppermute(last, axis, up)
        after = lax.ppermute(initial, axis, down)
        array = jnp.concatenate([before, array, after], axis=dim)
    return array


def level_coefficients(per_level_values):
    spread = DIFFUSE / 4.0**per_level_values
    drifts = tuple((component / 2.0**per_level_values for component in ADVECT))
    return (spread, drifts)


def pad_second(volume, position):
    widths = [(0, 0)] * volume.ndim
    widths[position] = (1, 1)
    return jnp.pad(volume, widths)


def apply_operator(padded, current_capacity, spectral_shifts, per_level_values):
    spread, drifts = level_coefficients(per_level_values)
    centre = padded[:, :, 1:-1]
    upper_first = padded[:, :, 2:]
    lower_first = padded[:, :, :-2]
    wide_second = pad_second(centre, 3)
    upper_second = wide_second[:, :, :, 2:]
    lower_second = wide_second[:, :, :, :-2]
    wide_third = pad_second(centre, 4)
    upper_third = wide_third[:, :, :, :, 2:]
    lower_third = wide_third[:, :, :, :, :-2]
    stencil = spread * (
        6.0 * centre
        - upper_first
        - lower_first
        - upper_second
        - lower_second
        - upper_third
        - lower_third
    )
    stencil = (
        stencil
        + drifts[0] * (upper_first - lower_first)
        + drifts[1] * (upper_second - lower_second)
        + drifts[2] * (upper_third - lower_third)
    )
    first_shift, second_shift, third_shift = spectral_shifts
    real_part = centre[0]
    imag_part = centre[1]
    shifted = jnp.stack(
        [
            current_capacity * (first_shift * real_part - second_shift * imag_part),
            current_capacity * (second_shift * real_part + third_shift * imag_part),
        ]
    )
    return stencil + shifted


def inverse_diagonal(current_capacity, spectral_shifts, per_level_values):
    spread, drifts = level_coefficients(per_level_values)
    first_shift, second_shift, third_shift = spectral_shifts
    top_left = current_capacity * first_shift + 6.0 * spread
    coupling = current_capacity * second_shift
    bottom_right = current_capacity * third_shift + 6.0 * spread
    determinant = top_left * bottom_right + coupling * coupling
    return (bottom_right / determinant, coupling / determinant, top_left / determinant)


def damped_update(residual_now, inverse):
    diagonal_a, diagonal_b, diagonal_c = inverse
    return OMEGA * jnp.stack(
        [
            diagonal_a * residual_now[0] + diagonal_b * residual_now[1],
            diagonal_c * residual_now[1] - diagonal_b * residual_now[0],
        ]
    )


def restrict_to_coarse(volume):
    leading = volume.shape[:-3]
    first_extent, second_extent, third_extent = volume.shape[-3:]
    blocks = volume.reshape(
        leading + (first_extent // 2, 2, second_extent // 2, 2, third_extent // 2, 2)
    )
    lead_count = len(leading)
    return jnp.mean(blocks, axis=(lead_count + 1, lead_count + 3, lead_count + 5))


def prolong_cells(volume):
    leading = volume.shape[:-3]
    first_extent, second_extent, third_extent = volume.shape[-3:]
    expanded = jnp.broadcast_to(
        volume[..., :, None, :, None, :, None],
        leading + (first_extent, 2, second_extent, 2, third_extent, 2),
    )
    return expanded.reshape(leading + (2 * first_extent, 2 * second_extent, 2 * third_extent))


def shift_values(frequency, length):
    ratio_step = ALPHA_CORNER ** (1.0 / length)
    phases = 2.0 * math.pi / length * frequency.astype(jnp.float32)
    first_shift = (1.0 - ratio_step * jnp.cos(phases)) / STEP_SIZE
    second_shift = ratio_step * jnp.sin(phases) / STEP_SIZE
    leading = frequency == 0
    second_shift = jnp.where(leading, 0.0, second_shift)
    third_shift = jnp.where(leading, (1.0 + ratio_step) / STEP_SIZE, first_shift)
    return tuple(
        (column.reshape(-1, 1, 1, 1) for column in (first_shift, second_shift, third_shift))
    )


def phase_grid(row_count, length):
    integers = (
        jnp.arange(row_count, dtype=jnp.int32)[:, None]
        * jnp.arange(length, dtype=jnp.int32)[None, :]
        % length
    )
    return 2.0 * math.pi / length * integers.astype(jnp.float32)


def pad_faces(volume):
    return extended(volume, (("space", 2),), 1)


def multigrid_cycle(
    per_level_values,
    forcing_term,
    capacity_fields,
    spectral_shifts,
    shared_values,
    assemble_level,
    assemble_parts,
):
    current_capacity = capacity_fields[per_level_values]
    inverse = inverse_diagonal(current_capacity, spectral_shifts, per_level_values)
    coarsest = per_level_values == GRID_DEPTH - 1
    current = damped_update(forcing_term, inverse)
    for repeat in range((COARSE_SWEEPS if coarsest else SMOOTH) - 1):
        current = current + damped_update(
            forcing_term
            - apply_operator(
                pad_faces(current), current_capacity, spectral_shifts, per_level_values
            ),
            inverse,
        )
    if coarsest:
        return current
    coarse_right_hand = restrict_to_coarse(
        forcing_term
        - apply_operator(pad_faces(current), current_capacity, spectral_shifts, per_level_values)
    )
    coarse_solution = multigrid_cycle(
        per_level_values + 1,
        coarse_right_hand,
        capacity_fields,
        spectral_shifts,
        shared_values,
        assemble_level,
        assemble_parts,
    )
    current = current + prolong_cells(coarse_solution)
    for repeat in range(SMOOTH):
        current = current + damped_update(
            forcing_term
            - apply_operator(
                pad_faces(current), current_capacity, spectral_shifts, per_level_values
            ),
            inverse,
        )
    return current


def on_device(residual, capacity):
    steps_here, thickness, extent_second, extent_third = residual.shape
    length = lax.axis_size("tm") * steps_here
    ratio_step = ALPHA_CORNER ** (1.0 / length)
    moments = (lax.axis_index("tm") * steps_here + jnp.arange(steps_here, dtype=jnp.int32)).astype(
        jnp.float32
    )
    scaled = (residual * jnp.power(ratio_step, moments)[:, None, None, None]).reshape(
        steps_here, -1
    )
    series = lax.all_to_all(scaled, "tm", split_axis=1, concat_axis=0, tiled=True)
    all_weights = jnp.power(ratio_step, jnp.arange(length, dtype=jnp.float32))
    alternate = 1.0 - 2.0 * (jnp.arange(length, dtype=jnp.int32) % 2).astype(jnp.float32)
    capacity_fields = [capacity]
    for per_level_values in range(1, GRID_DEPTH):
        capacity_fields.append(restrict_to_coarse(capacity_fields[-1]))
    halves = length // 2
    phases = phase_grid(halves, length)
    first_row = jnp.arange(halves, dtype=jnp.int32)[:, None] == 0
    forward = jnp.concatenate(
        [jnp.cos(phases), jnp.where(first_row, alternate[None, :], -jnp.sin(phases))], axis=0
    )
    spectrum = jnp.dot(forward, series, precision=HIGHEST).reshape(2, halves, -1)
    received = lax.all_to_all(spectrum, "tm", split_axis=1, concat_axis=2, tiled=True)
    slot_count = steps_here // 2
    frequency = lax.axis_index("tm") * slot_count + jnp.arange(slot_count, dtype=jnp.int32)
    spectral_shifts = shift_values(frequency, length)
    field_list = received.reshape(2, slot_count, thickness, extent_second, extent_third)
    solved_fields = multigrid_cycle(
        0, field_list, capacity_fields, spectral_shifts, False, GRID_DEPTH, None
    )
    flattened = solved_fields.reshape(2, slot_count, -1)
    returned = lax.all_to_all(flattened, "tm", split_axis=2, concat_axis=1, tiled=True)
    halves = length // 2
    phases = jnp.transpose(phase_grid(halves, length))
    first_column = jnp.arange(halves, dtype=jnp.int32)[None, :] == 0
    real_columns = jnp.where(first_column, 1.0, 2.0 * jnp.cos(phases)) / length
    imag_columns = jnp.where(first_column, alternate[:, None], -2.0 * jnp.sin(phases)) / length
    inverse_table = jnp.concatenate([real_columns, imag_columns], axis=1)
    values = jnp.dot(
        inverse_table,
        returned.reshape(returned.shape[0] * returned.shape[1], -1),
        precision=HIGHEST,
    )
    values = values / all_weights[:, None]
    result = lax.all_to_all(values, "tm", split_axis=0, concat_axis=1, tiled=True)
    return result.reshape(residual.shape)


MESH = pl.DeviceIdType.MESH


def real_transform(values):
    count = len(values)
    if count == 1:
        return [(values[0], None)]
    evens, odds = real_transform(values[0::2]), real_transform(values[1::2])
    half = count // 2
    if count == 2:
        return [(evens[0][0] + odds[0][0], None), (evens[0][0] - odds[0][0], None)]
    found = [None] * (half + 1)
    found[0] = (evens[0][0] + odds[0][0], None)
    found[half] = (evens[0][0] - odds[0][0], None)
    found[half // 2] = (evens[half // 2][0], -odds[half // 2][0])
    for k in range(1, half // 2):
        cosine, sine = math.cos(2 * math.pi * k / count), -math.sin(2 * math.pi * k / count)
        (er, ei), (or_, oi) = evens[k], odds[k]
        tr, ti = cosine * or_ - sine * oi, cosine * oi + sine * or_
        found[k] = (er + tr, ei + ti)
        found[half - k] = (er - tr, ti - ei)
    return found


def real_inverse(modes):
    half = len(modes) - 1
    if half == 0:
        return [modes[0][0]]
    count = 2 * half
    if half == 1:
        return [modes[0][0] + modes[1][0], modes[0][0] - modes[1][0]]
    evens, odds = [None] * (half // 2 + 1), [None] * (half // 2 + 1)
    evens[0] = (modes[0][0] + modes[half][0], None)
    odds[0] = (modes[0][0] - modes[half][0], None)
    middle = modes[half // 2]
    evens[half // 2] = (2.0 * middle[0], None)
    odds[half // 2] = (-2.0 * middle[1], None)
    for k in range(1, half // 2):
        cosine, sine = math.cos(2 * math.pi * k / count), math.sin(2 * math.pi * k / count)
        (ar, ai), (br, bi) = modes[k], modes[half - k]
        dr, di = ar - br, ai + bi
        evens[k] = (ar + br, ai - bi)
        odds[k] = (cosine * dr - sine * di, cosine * di + sine * dr)
    first, second = real_inverse(evens), real_inverse(odds)
    return [part for pair in zip(first, second) for part in pair]


def pair_sum(value, distance):
    for axis in (-2, -1):
        dim = value.ndim + axis
        extent = value.shape[dim]
        upper = pltpu.roll(value, extent - distance, dim)
        lower = pltpu.roll(value, distance, dim)
        place = lax.broadcasted_iota(jnp.int32, value.shape, dim)
        value = value + jnp.where((place // distance) % 2 == 0, upper, lower)
    return value


def block_mean(value, distance):
    shape = (value.shape[0] // 2, 2) + value.shape[1:]
    paired = value.reshape(shape)
    return 0.125 * pair_sum(paired[:, 0] + paired[:, 1], distance)


def neighbour_weights(level, shape):
    spread, drifts = level_coefficients(level)
    distance = 2**level
    along_first = (drifts[0] - spread, -drifts[0] - spread)
    masked = []
    for dim in (0, 1):
        place = lax.broadcasted_iota(jnp.int32, shape, dim)
        upper = jnp.where(place < shape[dim] - distance, drifts[dim + 1] - spread, 0.0)
        lower = jnp.where(place >= distance, -drifts[dim + 1] - spread, 0.0)
        masked.append((upper, lower))
    return along_first, masked, distance


def neighbours(wide, weights):
    along_first, masked, distance = weights
    centre = wide[1:-1]
    total = along_first[0] * wide[2:] + along_first[1] * wide[:-2]
    for dim in (0, 1):
        extent = centre.shape[dim + 1]
        if distance >= extent:
            continue
        upper, lower = masked[dim]
        total = total + upper[None] * pltpu.roll(centre, extent - distance, dim + 1)
        total = total + lower[None] * pltpu.roll(centre, distance, dim + 1)
    return total


def blocks_of(extent, largest, body):
    block = min(extent, largest)

    def step(i, carry):
        body(pl.multiple_of(i * block, block), block)
        return carry

    if extent == block:
        body(0, block)
    else:
        lax.fori_loop(0, extent // block, step, 0)


BLOCK = 32


def prepare_level(level, caps, inverses, shifts):
    spread, unused = level_coefficients(level)
    s1, s2, s3 = shifts

    def body(start, block):
        cap = caps[level][pl.ds(start, block)]
        top, coupling, bottom = cap * s1 + 6.0 * spread, cap * s2, cap * s3 + 6.0 * spread
        scale = OMEGA / (top * bottom + coupling * coupling)
        inverses[level][pl.ds(start, block), 0] = bottom * scale
        inverses[level][pl.ds(start, block), 1] = coupling * scale
        inverses[level][pl.ds(start, block), 2] = top * scale
        if level + 1 < GRID_DEPTH:
            half = block // 2
            caps[level + 1][pl.ds(start // 2, half)] = block_mean(cap, 2**level)

    blocks_of(caps[level].shape[0], BLOCK, body)


def smooth_first(forcing, target, inverse):
    def body(start, block):
        here = pl.ds(start, block)
        a, b, c = inverse[here, 0], inverse[here, 1], inverse[here, 2]
        re, im = forcing[here, 0], forcing[here, 1]
        there = pl.ds(start + 1, block)
        target[there, 0] = a * re + b * im
        target[there, 1] = c * im - b * re

    blocks_of(forcing.shape[0], BLOCK, body)


def smooth(forcing, source, target, inverse, weights, offset=1, coarse=None):
    def body(start, block):
        here = pl.ds(start, block)
        wide_re = source[pl.ds(start, block + 2), 0]
        wide_im = source[pl.ds(start, block + 2), 1]
        r0 = forcing[here, 0] - neighbours(wide_re, weights)
        r1 = forcing[here, 1] - neighbours(wide_im, weights)
        a, b, c = inverse[here, 0], inverse[here, 1], inverse[here, 2]
        there = pl.ds(start + offset, block)
        target[there, 0] = (1.0 - OMEGA) * wide_re[1:-1] + (a * r0 + b * r1)
        target[there, 1] = (1.0 - OMEGA) * wide_im[1:-1] + (c * r1 - b * r0)

    blocks_of(forcing.shape[0], BLOCK, body)


def restrict_residual(level, forcing, source, cap, shifts, weights, target):
    spread, unused = level_coefficients(level)
    s1, s2, s3 = shifts

    def body(start, block):
        here = pl.ds(start, block)
        wide_re = source[pl.ds(start, block + 2), 0]
        wide_im = source[pl.ds(start, block + 2), 1]
        re, im = wide_re[1:-1], wide_im[1:-1]
        field = cap[here]
        r0 = forcing[here, 0] - neighbours(wide_re, weights)
        r1 = forcing[here, 1] - neighbours(wide_im, weights)
        r0 = r0 - (6.0 * spread * re + field * (s1 * re - s2 * im))
        r1 = r1 - (6.0 * spread * im + field * (s2 * re + s3 * im))
        half = pl.ds(start // 2, block // 2)
        target[half, 0] = block_mean(r0, 2**level)
        target[half, 1] = block_mean(r1, 2**level)

    blocks_of(forcing.shape[0], BLOCK, body)


def add_coarse(target, coarse):
    def body(start, block):
        half = block // 2
        for part in (0, 1):
            extra = coarse[pl.ds(start // 2 + 1, half), part]
            spread = jnp.broadcast_to(extra[:, None], (half, 2) + extra.shape[1:])
            there = pl.ds(start + 1, block)
            target[there, part] = target[there, part] + spread.reshape((block,) + extra.shape[1:])

    blocks_of(target.shape[0] - 2, BLOCK, body)


def cycle(level, forcings, caps, inverses, firsts, seconds, shifts, result):
    forcing, inverse = forcings[level], inverses[level]
    here, other = firsts[level], seconds[level]
    weights = neighbour_weights(level, forcing.shape[-2:])
    coarsest = level == GRID_DEPTH - 1
    smooth_first(forcing, here, inverse)
    for repeat in range((COARSE_SWEEPS if coarsest else SMOOTH) - 1):
        smooth(forcing, here, other, inverse, weights)
        here, other = other, here
    if coarsest:
        return here
    restrict_residual(level, forcing, here, caps[level], shifts, weights, forcings[level + 1])
    coarse = cycle(level + 1, forcings, caps, inverses, firsts, seconds, shifts, None)
    add_coarse(here, coarse)
    for repeat in range(SMOOTH):
        last = repeat == SMOOTH - 1 and result is not None
        target = result if last else other
        smooth(forcing, here, target, inverse, weights, offset=0 if last else 1)
        here, other = target, here
    return here


def whole_kernel(groups, slabs, shift_table, residual_hbm, capacity_hbm, out_ref, *scratch):
    (series, spectrum, returned, values, result) = scratch[:5]
    residual_ref = scratch[-1]
    scratch = scratch[:-1]
    depth = GRID_DEPTH
    forcings = scratch[5 : 5 + depth]
    caps = scratch[5 + depth : 5 + 2 * depth]
    inverses = scratch[5 + 2 * depth : 5 + 3 * depth]
    firsts = scratch[5 + 3 * depth : 5 + 4 * depth]
    seconds = scratch[5 + 4 * depth : 5 + 5 * depth]
    send1, recv1, send2, recv2, send3, recv3, send4, recv4, own, sendc, recvc, ready = scratch[
        5 + 5 * depth :
    ]
    steps, thick = residual_ref.shape[:2]
    planes = thick // groups
    length = groups * steps
    devices = groups * slabs
    ratio_step = ALPHA_CORNER ** (1.0 / length)
    mine, slab = lax.axis_index("tm"), lax.axis_index("space")
    me = mine * slabs + slab
    base = slab * thick + mine * planes

    def peer_of(k):
        to_tm = lax.rem(mine + k, groups)
        to_space = lax.rem(slab + k // groups, slabs)
        return to_tm * slabs + to_space, to_tm, to_space

    own_slab = pl.ds(slab * thick, thick)
    take_residual = pltpu.make_async_copy(residual_hbm, residual_ref, own.at[3 * planes])
    take_capacity = pltpu.make_async_copy(
        capacity_hbm, caps[0].at[own_slab], own.at[3 * planes + 1]
    )
    take_residual.start()
    take_capacity.start()
    barrier = pltpu.get_barrier_semaphore()

    partner = slab + 1 - 2 * lax.rem(slab, 2)
    below, above = slab >= 2, slab < slabs - 2
    sides = jnp.where(below, 1, 0) + jnp.where(above, 1, 0)

    def tell_sides(semaphore):
        for there, step in ((below, -2), (above, 2)):

            @pl.when(there)
            def _():
                pl.semaphore_signal(
                    semaphore, inc=1, device_id=(mine, slab + step), device_id_type=MESH
                )

    for d in range(1, groups):
        pl.semaphore_signal(
            barrier, inc=1, device_id=(lax.rem(mine + d, groups), slab), device_id_type=MESH
        )
    tell_sides(barrier)
    pl.semaphore_signal(barrier, inc=1, device_id=(mine, partner), device_id_type=MESH)
    for level in range(depth):
        for buffer in (firsts[level], seconds[level]):
            empty = jnp.zeros(buffer.shape[1:], jnp.float32)
            buffer[0] = empty
            buffer[buffer.shape[0] - 1] = empty
    take_residual.wait()
    pl.semaphore_wait(barrier, groups + sides)

    first_sends = []
    for p in range(planes):
        for d in range(1, groups):
            to_tm = lax.rem(mine + d, groups)
            copy = pltpu.make_async_remote_copy(
                src_ref=residual_ref.at[:, to_tm * planes + p],
                dst_ref=series.at[p, pl.ds(mine * steps, steps)],
                send_sem=send1.at[p, d],
                recv_sem=recv1.at[p, d],
                device_id=(to_tm, slab),
                device_id_type=MESH,
            )
            copy.start()
            first_sends.append(copy)
    own_steps = []
    for p in range(planes):
        copy = pltpu.make_async_copy(
            residual_ref.at[:, mine * planes + p],
            series.at[p, pl.ds(mine * steps, steps)],
            own.at[p],
        )
        copy.start()
        own_steps.append(copy)

    for turn in range(slabs // 2 - 1):
        tell_sides(ready.at[turn])
        pl.semaphore_wait(ready.at[turn], sides)
    last = slabs // 2 - 1
    pl.semaphore_signal(ready.at[last], inc=1, device_id=(mine, partner), device_id_type=MESH)
    pl.semaphore_wait(ready.at[last], 1)

    take_capacity.wait()
    cap_sends = []
    for d in range(1, slabs // 2):
        copy = pltpu.make_async_remote_copy(
            src_ref=caps[0].at[own_slab],
            dst_ref=caps[0].at[own_slab],
            send_sem=sendc.at[d],
            recv_sem=recvc.at[d],
            device_id=(mine, lax.rem(slab + 2 * d, slabs)),
            device_id_type=MESH,
        )
        copy.start()
        cap_sends.append(copy)

    def forward_cap(d):
        index = lax.rem(slab + slabs - 2 * d, slabs)
        rows = pl.ds(index * thick, thick)
        copy = pltpu.make_async_remote_copy(
            src_ref=caps[0].at[rows],
            dst_ref=caps[0].at[rows],
            send_sem=sendc.at[slabs // 2 + d],
            recv_sem=recvc.at[slabs // 2 + d],
            device_id=(mine, partner),
            device_id_type=MESH,
        )
        copy.start()
        return copy

    cap_forwards = [forward_cap(0)]

    def spread_mode(k, p):
        peer, to_tm, to_space = peer_of(k)
        return pltpu.make_async_remote_copy(
            src_ref=spectrum.at[p, peer],
            dst_ref=forcings[0].at[base + p],
            send_sem=send2.at[p],
            recv_sem=recv2.at[p],
            device_id=(to_tm, to_space),
            device_id_type=MESH,
        )

    own_modes = []
    for p in range(planes):
        own_steps[p].wait()
        for d in range(1, groups):
            first_sends[p * (groups - 1) + d - 1].wait_recv()
        modes = real_transform([ratio_step**t * series[p, t] for t in range(length)])
        spectrum[p, 0, 0] = modes[0][0]
        spectrum[p, 0, 1] = modes[length // 2][0]
        for k in range(1, length // 2):
            spectrum[p, k, 0] = modes[k][0]
            spectrum[p, k, 1] = modes[k][1]

        def start_mode(k, carry):
            spread_mode(k, p).start()
            return carry

        lax.fori_loop(1, devices, start_mode, 0)
        copy = pltpu.make_async_copy(
            spectrum.at[p, me], forcings[0].at[base + p], own.at[planes + p]
        )
        copy.start()
        own_modes.append(copy)
        if p == 0:
            for d in range(1, slabs // 2):
                cap_sends[d - 1].wait_recv()
                cap_forwards.append(forward_cap(d))

    for copy in cap_forwards:
        copy.wait_recv()
    shifts = []
    for column in range(3):
        value = jnp.float32(shift_table[0, column])
        for k in range(1, devices):
            value = jnp.where(me == k, jnp.float32(shift_table[k, column]), value)
        shifts.append(value)
    for level in range(depth):
        prepare_level(level, caps, inverses, shifts)

    def all_but_one(array, semaphore):
        part = array.at[pl.ds(0, devices - 1)]
        return pltpu.make_async_copy(part, part, semaphore)

    for p in range(planes):
        own_modes[p].wait()
        all_but_one(forcings[0], recv2.at[p]).wait()

    cycle(0, forcings, caps, inverses, firsts, seconds, shifts, result)

    def send_back(k, p):
        peer, to_tm, to_space = peer_of(k)
        return pltpu.make_async_remote_copy(
            src_ref=result.at[to_space * thick + to_tm * planes + p],
            dst_ref=returned.at[p, me],
            send_sem=send3.at[p],
            recv_sem=recv3.at[p],
            device_id=(to_tm, to_space),
            device_id_type=MESH,
        )

    own_back = []
    for p in range(planes):

        def start_back(k, carry):
            send_back(k, p).start()
            return carry

        lax.fori_loop(1, devices, start_back, 0)
        copy = pltpu.make_async_copy(
            result.at[base + p], returned.at[p, me], own.at[2 * planes + p]
        )
        copy.start()
        own_back.append(copy)

    last_copies = []
    for p in range(planes):
        own_back[p].wait()
        all_but_one(returned.at[p], recv3.at[p]).wait()
        modes = [(returned[p, 0, 0], None)]
        modes += [(returned[p, k, 0], returned[p, k, 1]) for k in range(1, length // 2)]
        modes += [(returned[p, 0, 1], None)]
        for t, value in enumerate(real_inverse(modes)):
            values[p, t] = value * (ratio_step**-t / length)
        for d in range(1, groups):
            to_tm = lax.rem(mine + d, groups)
            copy = pltpu.make_async_remote_copy(
                src_ref=values.at[p, pl.ds(to_tm * steps, steps)],
                dst_ref=out_ref.at[:, mine * planes + p],
                send_sem=send4.at[p, d],
                recv_sem=recv4.at[p, d],
                device_id=(to_tm, slab),
                device_id_type=MESH,
            )
            copy.start()
            last_copies.append(copy)
        out_ref[:, mine * planes + p] = values[p, pl.ds(mine * steps, steps)]

    for copy in last_copies:
        copy.wait()
    for copy in first_sends + cap_sends + cap_forwards:
        copy.wait_send()
    for p in range(planes):
        all_but_one(spectrum.at[p], send2.at[p]).wait()
        all_but_one(result, send3.at[p]).wait()


def level_extents(extent):
    return [extent // 2**level for level in range(GRID_DEPTH)]


def fused(groups, slabs, residual, capacity):
    steps, thick, second, third = residual.shape
    length, devices = groups * steps, groups * slabs
    planes, extent = thick // groups, slabs * thick
    tile = (second, third)
    ratio_step = ALPHA_CORNER ** (1.0 / length)
    angle = 2.0 * np.pi / length * np.arange(devices)
    table = np.stack(
        [
            (1.0 - ratio_step * np.cos(angle)) / STEP_SIZE,
            ratio_step * np.sin(angle) / STEP_SIZE,
            (1.0 - ratio_step * np.cos(angle)) / STEP_SIZE,
        ],
        axis=1,
    )
    table[0, 1], table[0, 2] = 0.0, (1.0 + ratio_step) / STEP_SIZE
    extents = level_extents(extent)
    vmem = lambda *shape: pltpu.VMEM(shape + tile, jnp.float32)
    sems = lambda *shape: pltpu.SemaphoreType.DMA(shape)
    scratch = [
        vmem(planes, length),
        vmem(planes, devices, 2),
        vmem(planes, devices, 2),
        vmem(planes, length),
        vmem(extent, 2),
        *[vmem(n, 2) for n in extents],
        *[vmem(n) for n in extents],
        *[vmem(n, 3) for n in extents],
        *[vmem(n + 2, 2) for n in extents],
        *[vmem(n + 2, 2) for n in extents],
        sems(planes, groups),
        sems(planes, groups),
        sems(planes),
        sems(planes),
        sems(planes),
        sems(planes),
        sems(planes, groups),
        sems(planes, groups),
        sems(3 * planes + 2),
        sems(slabs),
        sems(slabs),
        pltpu.SemaphoreType.REGULAR((slabs // 2,)),
        pltpu.VMEM(residual.shape, jnp.float32),
    ]
    return pl.pallas_call(
        functools.partial(whole_kernel, groups, slabs, table),
        out_shape=jax.ShapeDtypeStruct(residual.shape, jnp.float32),
        in_specs=[
            pl.BlockSpec(memory_space=pltpu.HBM),
            pl.BlockSpec(memory_space=pltpu.HBM),
        ],
        out_specs=pl.BlockSpec(memory_space=pltpu.VMEM),
        scratch_shapes=scratch,
        compiler_params=pltpu.CompilerParams(
            collective_id=0, has_side_effects=True, vmem_limit_bytes=32 * 2**20
        ),
    )(residual, capacity)


def fits_fused(groups, slabs, residual):
    steps, thick, second, third = residual.shape
    length = groups * steps
    power = length & (length - 1) == 0
    return (
        power
        and groups * slabs == length // 2
        and slabs % 2 == 0
        and thick % groups == 0
        and all(n % 2 == 0 and n % min(n, BLOCK) == 0 for n in level_extents(slabs * thick))
        and (second, third) == (8, 128)
    )


def either(residual, capacity):
    groups, slabs = lax.axis_size("tm"), lax.axis_size("space")
    if fits_fused(groups, slabs, residual):
        return fused(groups, slabs, residual, capacity)
    return on_device(residual, capacity)


def solution(mesh):
    return jax.shard_map(
        either,
        mesh=mesh,
        in_specs=(P("tm", "space", None, None), P("space", None, None)),
        out_specs=P("tm", "space", None, None),
        check_vma=False,
    )
```

```python
import functools
import math

import jax
import jax.numpy as jnp
import numpy as np
from jax import lax
from jax.experimental import pallas as pl
from jax.experimental.pallas import tpu as pltpu
from jax.sharding import PartitionSpec as P

GRID_DEPTH = 4
SMOOTH = 2
COARSE_SWEEPS = 6


ALPHA_CORNER = 0.01
STEP_SIZE = 0.5
DIFFUSE = 2.0
ADVECT = (0.2, -0.15, 0.1)
OMEGA = 0.7
HIGHEST = lax.Precision.HIGHEST


def extended(array, sides, width):
    for axis, dim in sides:
        peers, length = (lax.axis_size(axis), array.shape[dim])
        up = [(i, (i + 1) % peers) for i in range(peers - 1)]
        down = [(j, i) for i, j in up]
        last = lax.slice_in_dim(array, length - width, length, axis=dim)
        initial = lax.slice_in_dim(array, 0, width, axis=dim)
        before = lax.ppermute(last, axis, up)
        after = lax.ppermute(initial, axis, down)
        array = jnp.concatenate([before, array, after], axis=dim)
    return array


def level_coefficients(per_level_values):
    spread = DIFFUSE / 4.0**per_level_values
    drifts = tuple((component / 2.0**per_level_values for component in ADVECT))
    return (spread, drifts)


def pad_second(volume, position):
    widths = [(0, 0)] * volume.ndim
    widths[position] = (1, 1)
    return jnp.pad(volume, widths)


def apply_operator(padded, current_capacity, spectral_shifts, per_level_values):
    spread, drifts = level_coefficients(per_level_values)
    centre = padded[:, :, 1:-1]
    upper_first = padded[:, :, 2:]
    lower_first = padded[:, :, :-2]
    wide_second = pad_second(centre, 3)
    upper_second = wide_second[:, :, :, 2:]
    lower_second = wide_second[:, :, :, :-2]
    wide_third = pad_second(centre, 4)
    upper_third = wide_third[:, :, :, :, 2:]
    lower_third = wide_third[:, :, :, :, :-2]
    stencil = spread * (
        6.0 * centre
        - upper_first
        - lower_first
        - upper_second
        - lower_second
        - upper_third
        - lower_third
    )
    stencil = (
        stencil
        + drifts[0] * (upper_first - lower_first)
        + drifts[1] * (upper_second - lower_second)
        + drifts[2] * (upper_third - lower_third)
    )
    first_shift, second_shift, third_shift = spectral_shifts
    real_part = centre[0]
    imag_part = centre[1]
    shifted = jnp.stack(
        [
            current_capacity * (first_shift * real_part - second_shift * imag_part),
            current_capacity * (second_shift * real_part + third_shift * imag_part),
        ]
    )
    return stencil + shifted


def inverse_diagonal(current_capacity, spectral_shifts, per_level_values):
    spread, drifts = level_coefficients(per_level_values)
    first_shift, second_shift, third_shift = spectral_shifts
    top_left = current_capacity * first_shift + 6.0 * spread
    coupling = current_capacity * second_shift
    bottom_right = current_capacity * third_shift + 6.0 * spread
    determinant = top_left * bottom_right + coupling * coupling
    return (bottom_right / determinant, coupling / determinant, top_left / determinant)


def damped_update(residual_now, inverse):
    diagonal_a, diagonal_b, diagonal_c = inverse
    return OMEGA * jnp.stack(
        [
            diagonal_a * residual_now[0] + diagonal_b * residual_now[1],
            diagonal_c * residual_now[1] - diagonal_b * residual_now[0],
        ]
    )


def restrict_to_coarse(volume):
    leading = volume.shape[:-3]
    first_extent, second_extent, third_extent = volume.shape[-3:]
    blocks = volume.reshape(
        leading + (first_extent // 2, 2, second_extent // 2, 2, third_extent // 2, 2)
    )
    lead_count = len(leading)
    return jnp.mean(blocks, axis=(lead_count + 1, lead_count + 3, lead_count + 5))


def prolong_cells(volume):
    leading = volume.shape[:-3]
    first_extent, second_extent, third_extent = volume.shape[-3:]
    expanded = jnp.broadcast_to(
        volume[..., :, None, :, None, :, None],
        leading + (first_extent, 2, second_extent, 2, third_extent, 2),
    )
    return expanded.reshape(leading + (2 * first_extent, 2 * second_extent, 2 * third_extent))


def shift_values(frequency, length):
    ratio_step = ALPHA_CORNER ** (1.0 / length)
    phases = 2.0 * math.pi / length * frequency.astype(jnp.float32)
    first_shift = (1.0 - ratio_step * jnp.cos(phases)) / STEP_SIZE
    second_shift = ratio_step * jnp.sin(phases) / STEP_SIZE
    leading = frequency == 0
    second_shift = jnp.where(leading, 0.0, second_shift)
    third_shift = jnp.where(leading, (1.0 + ratio_step) / STEP_SIZE, first_shift)
    return tuple(
        (column.reshape(-1, 1, 1, 1) for column in (first_shift, second_shift, third_shift))
    )


def phase_grid(row_count, length):
    integers = (
        jnp.arange(row_count, dtype=jnp.int32)[:, None]
        * jnp.arange(length, dtype=jnp.int32)[None, :]
        % length
    )
    return 2.0 * math.pi / length * integers.astype(jnp.float32)


def pad_faces(volume):
    return extended(volume, (("space", 2),), 1)


def multigrid_cycle(
    per_level_values,
    forcing_term,
    capacity_fields,
    spectral_shifts,
    shared_values,
    assemble_level,
    assemble_parts,
):
    current_capacity = capacity_fields[per_level_values]
    inverse = inverse_diagonal(current_capacity, spectral_shifts, per_level_values)
    coarsest = per_level_values == GRID_DEPTH - 1
    current = damped_update(forcing_term, inverse)
    for repeat in range((COARSE_SWEEPS if coarsest else SMOOTH) - 1):
        current = current + damped_update(
            forcing_term
            - apply_operator(
                pad_faces(current), current_capacity, spectral_shifts, per_level_values
            ),
            inverse,
        )
    if coarsest:
        return current
    coarse_right_hand = restrict_to_coarse(
        forcing_term
        - apply_operator(pad_faces(current), current_capacity, spectral_shifts, per_level_values)
    )
    coarse_solution = multigrid_cycle(
        per_level_values + 1,
        coarse_right_hand,
        capacity_fields,
        spectral_shifts,
        shared_values,
        assemble_level,
        assemble_parts,
    )
    current = current + prolong_cells(coarse_solution)
    for repeat in range(SMOOTH):
        current = current + damped_update(
            forcing_term
            - apply_operator(
                pad_faces(current), current_capacity, spectral_shifts, per_level_values
            ),
            inverse,
        )
    return current


def on_device(residual, capacity):
    steps_here, thickness, extent_second, extent_third = residual.shape
    length = lax.axis_size("tm") * steps_here
    ratio_step = ALPHA_CORNER ** (1.0 / length)
    moments = (lax.axis_index("tm") * steps_here + jnp.arange(steps_here, dtype=jnp.int32)).astype(
        jnp.float32
    )
    scaled = (residual * jnp.power(ratio_step, moments)[:, None, None, None]).reshape(
        steps_here, -1
    )
    series = lax.all_to_all(scaled, "tm", split_axis=1, concat_axis=0, tiled=True)
    all_weights = jnp.power(ratio_step, jnp.arange(length, dtype=jnp.float32))
    alternate = 1.0 - 2.0 * (jnp.arange(length, dtype=jnp.int32) % 2).astype(jnp.float32)
    capacity_fields = [capacity]
    for per_level_values in range(1, GRID_DEPTH):
        capacity_fields.append(restrict_to_coarse(capacity_fields[-1]))
    halves = length // 2
    phases = phase_grid(halves, length)
    first_row = jnp.arange(halves, dtype=jnp.int32)[:, None] == 0
    forward = jnp.concatenate(
        [jnp.cos(phases), jnp.where(first_row, alternate[None, :], -jnp.sin(phases))], axis=0
    )
    spectrum = jnp.dot(forward, series, precision=HIGHEST).reshape(2, halves, -1)
    received = lax.all_to_all(spectrum, "tm", split_axis=1, concat_axis=2, tiled=True)
    slot_count = steps_here // 2
    frequency = lax.axis_index("tm") * slot_count + jnp.arange(slot_count, dtype=jnp.int32)
    spectral_shifts = shift_values(frequency, length)
    field_list = received.reshape(2, slot_count, thickness, extent_second, extent_third)
    solved_fields = multigrid_cycle(
        0, field_list, capacity_fields, spectral_shifts, False, GRID_DEPTH, None
    )
    flattened = solved_fields.reshape(2, slot_count, -1)
    returned = lax.all_to_all(flattened, "tm", split_axis=2, concat_axis=1, tiled=True)
    halves = length // 2
    phases = jnp.transpose(phase_grid(halves, length))
    first_column = jnp.arange(halves, dtype=jnp.int32)[None, :] == 0
    real_columns = jnp.where(first_column, 1.0, 2.0 * jnp.cos(phases)) / length
    imag_columns = jnp.where(first_column, alternate[:, None], -2.0 * jnp.sin(phases)) / length
    inverse_table = jnp.concatenate([real_columns, imag_columns], axis=1)
    values = jnp.dot(
        inverse_table,
        returned.reshape(returned.shape[0] * returned.shape[1], -1),
        precision=HIGHEST,
    )
    values = values / all_weights[:, None]
    result = lax.all_to_all(values, "tm", split_axis=0, concat_axis=1, tiled=True)
    return result.reshape(residual.shape)


MESH = pl.DeviceIdType.MESH


def real_transform(values):
    count = len(values)
    if count == 1:
        return [(values[0], None)]
    evens, odds = real_transform(values[0::2]), real_transform(values[1::2])
    half = count // 2
    if count == 2:
        return [(evens[0][0] + odds[0][0], None), (evens[0][0] - odds[0][0], None)]
    found = [None] * (half + 1)
    found[0] = (evens[0][0] + odds[0][0], None)
    found[half] = (evens[0][0] - odds[0][0], None)
    found[half // 2] = (evens[half // 2][0], -odds[half // 2][0])
    for k in range(1, half // 2):
        cosine, sine = math.cos(2 * math.pi * k / count), -math.sin(2 * math.pi * k / count)
        (er, ei), (or_, oi) = evens[k], odds[k]
        tr, ti = cosine * or_ - sine * oi, cosine * oi + sine * or_
        found[k] = (er + tr, ei + ti)
        found[half - k] = (er - tr, ti - ei)
    return found


def real_inverse(modes):
    half = len(modes) - 1
    if half == 0:
        return [modes[0][0]]
    count = 2 * half
    if half == 1:
        return [modes[0][0] + modes[1][0], modes[0][0] - modes[1][0]]
    evens, odds = [None] * (half // 2 + 1), [None] * (half // 2 + 1)
    evens[0] = (modes[0][0] + modes[half][0], None)
    odds[0] = (modes[0][0] - modes[half][0], None)
    middle = modes[half // 2]
    evens[half // 2] = (2.0 * middle[0], None)
    odds[half // 2] = (-2.0 * middle[1], None)
    for k in range(1, half // 2):
        cosine, sine = math.cos(2 * math.pi * k / count), math.sin(2 * math.pi * k / count)
        (ar, ai), (br, bi) = modes[k], modes[half - k]
        dr, di = ar - br, ai + bi
        evens[k] = (ar + br, ai - bi)
        odds[k] = (cosine * dr - sine * di, cosine * di + sine * dr)
    first, second = real_inverse(evens), real_inverse(odds)
    return [part for pair in zip(first, second) for part in pair]


def pair_sum(value, distance):
    for axis in (-2, -1):
        dim = value.ndim + axis
        extent = value.shape[dim]
        upper = pltpu.roll(value, extent - distance, dim)
        lower = pltpu.roll(value, distance, dim)
        place = lax.broadcasted_iota(jnp.int32, value.shape, dim)
        value = value + jnp.where((place // distance) % 2 == 0, upper, lower)
    return value


def block_mean(value, distance):
    shape = (value.shape[0] // 2, 2) + value.shape[1:]
    paired = value.reshape(shape)
    return 0.125 * pair_sum(paired[:, 0] + paired[:, 1], distance)


def neighbour_weights(level, shape):
    spread, drifts = level_coefficients(level)
    distance = 2**level
    along_first = (drifts[0] - spread, -drifts[0] - spread)
    masked = []
    for dim in (0, 1):
        place = lax.broadcasted_iota(jnp.int32, shape, dim)
        upper = jnp.where(place < shape[dim] - distance, drifts[dim + 1] - spread, 0.0)
        lower = jnp.where(place >= distance, -drifts[dim + 1] - spread, 0.0)
        masked.append((upper, lower))
    return along_first, masked, distance


def neighbours(wide, weights):
    along_first, masked, distance = weights
    centre = wide[1:-1]
    total = along_first[0] * wide[2:] + along_first[1] * wide[:-2]
    for dim in (0, 1):
        extent = centre.shape[dim + 1]
        if distance >= extent:
            continue
        upper, lower = masked[dim]
        total = total + upper[None] * pltpu.roll(centre, extent - distance, dim + 1)
        total = total + lower[None] * pltpu.roll(centre, distance, dim + 1)
    return total


def blocks_of(extent, largest, body):
    block = min(extent, largest)

    def step(i, carry):
        body(pl.multiple_of(i * block, block), block)
        return carry

    if extent == block:
        body(0, block)
    else:
        lax.fori_loop(0, extent // block, step, 0)


BLOCK = 64


def prepare_level(level, caps, inverses, shifts):
    spread, unused = level_coefficients(level)
    s1, s2, s3 = shifts

    def body(start, block):
        cap = caps[level][pl.ds(start, block)]
        top, coupling, bottom = cap * s1 + 6.0 * spread, cap * s2, cap * s3 + 6.0 * spread
        scale = OMEGA / (top * bottom + coupling * coupling)
        inverses[level][pl.ds(start, block), 0] = bottom * scale
        inverses[level][pl.ds(start, block), 1] = coupling * scale
        inverses[level][pl.ds(start, block), 2] = top * scale
        if level + 1 < GRID_DEPTH:
            half = block // 2
            caps[level + 1][pl.ds(start // 2, half)] = block_mean(cap, 2**level)

    blocks_of(caps[level].shape[0], BLOCK, body)


def smooth_first(forcing, target, inverse):
    def body(start, block):
        here = pl.ds(start, block)
        a, b, c = inverse[here, 0], inverse[here, 1], inverse[here, 2]
        re, im = forcing[here, 0], forcing[here, 1]
        there = pl.ds(start + 1, block)
        target[there, 0] = a * re + b * im
        target[there, 1] = c * im - b * re

    blocks_of(forcing.shape[0], BLOCK, body)


def smooth(forcing, source, target, inverse, weights, offset=1, coarse=None):
    def body(start, block):
        here = pl.ds(start, block)
        wide_re = source[pl.ds(start, block + 2), 0]
        wide_im = source[pl.ds(start, block + 2), 1]
        r0 = forcing[here, 0] - neighbours(wide_re, weights)
        r1 = forcing[here, 1] - neighbours(wide_im, weights)
        a, b, c = inverse[here, 0], inverse[here, 1], inverse[here, 2]
        there = pl.ds(start + offset, block)
        target[there, 0] = (1.0 - OMEGA) * wide_re[1:-1] + (a * r0 + b * r1)
        target[there, 1] = (1.0 - OMEGA) * wide_im[1:-1] + (c * r1 - b * r0)

    blocks_of(forcing.shape[0], BLOCK, body)


def restrict_residual(level, forcing, source, cap, shifts, weights, target):
    spread, unused = level_coefficients(level)
    s1, s2, s3 = shifts

    def body(start, block):
        here = pl.ds(start, block)
        wide_re = source[pl.ds(start, block + 2), 0]
        wide_im = source[pl.ds(start, block + 2), 1]
        re, im = wide_re[1:-1], wide_im[1:-1]
        field = cap[here]
        r0 = forcing[here, 0] - neighbours(wide_re, weights)
        r1 = forcing[here, 1] - neighbours(wide_im, weights)
        r0 = r0 - (6.0 * spread * re + field * (s1 * re - s2 * im))
        r1 = r1 - (6.0 * spread * im + field * (s2 * re + s3 * im))
        half = pl.ds(start // 2, block // 2)
        target[half, 0] = block_mean(r0, 2**level)
        target[half, 1] = block_mean(r1, 2**level)

    blocks_of(forcing.shape[0], BLOCK, body)


def add_coarse(target, coarse):
    def body(start, block):
        half = block // 2
        for part in (0, 1):
            extra = coarse[pl.ds(start // 2 + 1, half), part]
            spread = jnp.broadcast_to(extra[:, None], (half, 2) + extra.shape[1:])
            there = pl.ds(start + 1, block)
            target[there, part] = target[there, part] + spread.reshape((block,) + extra.shape[1:])

    blocks_of(target.shape[0] - 2, BLOCK, body)


def cycle(level, forcings, caps, inverses, firsts, seconds, shifts, result):
    forcing, inverse = forcings[level], inverses[level]
    here, other = firsts[level], seconds[level]
    weights = neighbour_weights(level, forcing.shape[-2:])
    coarsest = level == GRID_DEPTH - 1
    smooth_first(forcing, here, inverse)
    for repeat in range((COARSE_SWEEPS if coarsest else SMOOTH) - 1):
        smooth(forcing, here, other, inverse, weights)
        here, other = other, here
    if coarsest:
        return here
    restrict_residual(level, forcing, here, caps[level], shifts, weights, forcings[level + 1])
    coarse = cycle(level + 1, forcings, caps, inverses, firsts, seconds, shifts, None)
    add_coarse(here, coarse)
    for repeat in range(SMOOTH):
        last = repeat == SMOOTH - 1 and result is not None
        target = result if last else other
        smooth(forcing, here, target, inverse, weights, offset=0 if last else 1)
        here, other = target, here
    return here


def whole_kernel(groups, slabs, shift_table, residual_hbm, capacity_hbm, out_ref, *scratch):
    (series, spectrum, returned, values, result) = scratch[:5]
    residual_ref = scratch[-1]
    scratch = scratch[:-1]
    depth = GRID_DEPTH
    forcings = scratch[5 : 5 + depth]
    caps = scratch[5 + depth : 5 + 2 * depth]
    inverses = scratch[5 + 2 * depth : 5 + 3 * depth]
    firsts = scratch[5 + 3 * depth : 5 + 4 * depth]
    seconds = scratch[5 + 4 * depth : 5 + 5 * depth]
    send1, recv1, send2, recv2, send3, recv3, send4, recv4, own, sendc, recvc, ready = scratch[
        5 + 5 * depth :
    ]
    steps, thick = residual_ref.shape[:2]
    planes = thick // groups
    length = groups * steps
    devices = groups * slabs
    ratio_step = ALPHA_CORNER ** (1.0 / length)
    mine, slab = lax.axis_index("tm"), lax.axis_index("space")
    me = mine * slabs + slab
    base = slab * thick + mine * planes

    def peer_of(k):
        to_tm = lax.rem(mine + k, groups)
        to_space = lax.rem(slab + k // groups, slabs)
        return to_tm * slabs + to_space, to_tm, to_space

    own_slab = pl.ds(slab * thick, thick)
    take_residual = pltpu.make_async_copy(residual_hbm, residual_ref, own.at[3 * planes])
    take_capacity = pltpu.make_async_copy(
        capacity_hbm, caps[0].at[own_slab], own.at[3 * planes + 1]
    )
    take_residual.start()
    take_capacity.start()
    barrier = pltpu.get_barrier_semaphore()

    partner = slab + 1 - 2 * lax.rem(slab, 2)
    below, above = slab >= 2, slab < slabs - 2
    sides = jnp.where(below, 1, 0) + jnp.where(above, 1, 0)

    def tell_sides(semaphore):
        for there, step in ((below, -2), (above, 2)):

            @pl.when(there)
            def _():
                pl.semaphore_signal(
                    semaphore, inc=1, device_id=(mine, slab + step), device_id_type=MESH
                )

    for d in range(1, groups):
        pl.semaphore_signal(
            barrier, inc=1, device_id=(lax.rem(mine + d, groups), slab), device_id_type=MESH
        )
    tell_sides(barrier)
    pl.semaphore_signal(barrier, inc=1, device_id=(mine, partner), device_id_type=MESH)
    for level in range(depth):
        for buffer in (firsts[level], seconds[level]):
            empty = jnp.zeros(buffer.shape[1:], jnp.float32)
            buffer[0] = empty
            buffer[buffer.shape[0] - 1] = empty
    take_residual.wait()
    pl.semaphore_wait(barrier, groups + sides)

    first_sends = []
    for p in range(planes):
        for d in range(1, groups):
            to_tm = lax.rem(mine + d, groups)
            copy = pltpu.make_async_remote_copy(
                src_ref=residual_ref.at[:, to_tm * planes + p],
                dst_ref=series.at[p, pl.ds(mine * steps, steps)],
                send_sem=send1.at[p, d],
                recv_sem=recv1.at[p, d],
                device_id=(to_tm, slab),
                device_id_type=MESH,
            )
            copy.start()
            first_sends.append(copy)
    own_steps = []
    for p in range(planes):
        copy = pltpu.make_async_copy(
            residual_ref.at[:, mine * planes + p],
            series.at[p, pl.ds(mine * steps, steps)],
            own.at[p],
        )
        copy.start()
        own_steps.append(copy)

    for turn in range(slabs // 2 - 1):
        tell_sides(ready.at[turn])
        pl.semaphore_wait(ready.at[turn], sides)
    last = slabs // 2 - 1
    pl.semaphore_signal(ready.at[last], inc=1, device_id=(mine, partner), device_id_type=MESH)
    pl.semaphore_wait(ready.at[last], 1)

    take_capacity.wait()
    cap_sends = []
    for d in range(1, slabs // 2):
        copy = pltpu.make_async_remote_copy(
            src_ref=caps[0].at[own_slab],
            dst_ref=caps[0].at[own_slab],
            send_sem=sendc.at[d],
            recv_sem=recvc.at[d],
            device_id=(mine, lax.rem(slab + 2 * d, slabs)),
            device_id_type=MESH,
        )
        copy.start()
        cap_sends.append(copy)

    def forward_cap(d):
        index = lax.rem(slab + slabs - 2 * d, slabs)
        rows = pl.ds(index * thick, thick)
        copy = pltpu.make_async_remote_copy(
            src_ref=caps[0].at[rows],
            dst_ref=caps[0].at[rows],
            send_sem=sendc.at[slabs // 2 + d],
            recv_sem=recvc.at[slabs // 2 + d],
            device_id=(mine, partner),
            device_id_type=MESH,
        )
        copy.start()
        return copy

    cap_forwards = [forward_cap(0)]

    def spread_mode(k, p):
        peer, to_tm, to_space = peer_of(k)
        return pltpu.make_async_remote_copy(
            src_ref=spectrum.at[p, peer],
            dst_ref=forcings[0].at[base + p],
            send_sem=send2.at[p],
            recv_sem=recv2.at[p],
            device_id=(to_tm, to_space),
            device_id_type=MESH,
        )

    own_modes = []
    for p in range(planes):
        own_steps[p].wait()
        for d in range(1, groups):
            first_sends[p * (groups - 1) + d - 1].wait_recv()
        modes = real_transform([ratio_step**t * series[p, t] for t in range(length)])
        spectrum[p, 0, 0] = modes[0][0]
        spectrum[p, 0, 1] = modes[length // 2][0]
        for k in range(1, length // 2):
            spectrum[p, k, 0] = modes[k][0]
            spectrum[p, k, 1] = modes[k][1]

        def start_mode(k, carry):
            spread_mode(k, p).start()
            return carry

        lax.fori_loop(1, devices, start_mode, 0)
        copy = pltpu.make_async_copy(
            spectrum.at[p, me], forcings[0].at[base + p], own.at[planes + p]
        )
        copy.start()
        own_modes.append(copy)

    for d in range(1, slabs // 2):
        cap_sends[d - 1].wait_recv()
        cap_forwards.append(forward_cap(d))
    for copy in cap_forwards:
        copy.wait_recv()
    shifts = []
    for column in range(3):
        value = jnp.float32(shift_table[0, column])
        for k in range(1, devices):
            value = jnp.where(me == k, jnp.float32(shift_table[k, column]), value)
        shifts.append(value)
    for level in range(depth):
        prepare_level(level, caps, inverses, shifts)

    def all_but_one(array, semaphore):
        part = array.at[pl.ds(0, devices - 1)]
        return pltpu.make_async_copy(part, part, semaphore)

    for p in range(planes):
        own_modes[p].wait()
        all_but_one(forcings[0], recv2.at[p]).wait()

    cycle(0, forcings, caps, inverses, firsts, seconds, shifts, result)

    def send_back(k, p):
        peer, to_tm, to_space = peer_of(k)
        return pltpu.make_async_remote_copy(
            src_ref=result.at[to_space * thick + to_tm * planes + p],
            dst_ref=returned.at[p, me],
            send_sem=send3.at[p],
            recv_sem=recv3.at[p],
            device_id=(to_tm, to_space),
            device_id_type=MESH,
        )

    own_back = []
    for p in range(planes):

        def start_back(k, carry):
            send_back(k, p).start()
            return carry

        lax.fori_loop(1, devices, start_back, 0)
        copy = pltpu.make_async_copy(
            result.at[base + p], returned.at[p, me], own.at[2 * planes + p]
        )
        copy.start()
        own_back.append(copy)

    last_copies = []
    for p in range(planes):
        own_back[p].wait()
        all_but_one(returned.at[p], recv3.at[p]).wait()
        modes = [(returned[p, 0, 0], None)]
        modes += [(returned[p, k, 0], returned[p, k, 1]) for k in range(1, length // 2)]
        modes += [(returned[p, 0, 1], None)]
        for t, value in enumerate(real_inverse(modes)):
            values[p, t] = value * (ratio_step**-t / length)
        for d in range(1, groups):
            to_tm = lax.rem(mine + d, groups)
            copy = pltpu.make_async_remote_copy(
                src_ref=values.at[p, pl.ds(to_tm * steps, steps)],
                dst_ref=out_ref.at[:, mine * planes + p],
                send_sem=send4.at[p, d],
                recv_sem=recv4.at[p, d],
                device_id=(to_tm, slab),
                device_id_type=MESH,
            )
            copy.start()
            last_copies.append(copy)
        out_ref[:, mine * planes + p] = values[p, pl.ds(mine * steps, steps)]

    for copy in last_copies:
        copy.wait()
    for copy in first_sends + cap_sends + cap_forwards:
        copy.wait_send()
    for p in range(planes):
        all_but_one(spectrum.at[p], send2.at[p]).wait()
        all_but_one(result, send3.at[p]).wait()


def level_extents(extent):
    return [extent // 2**level for level in range(GRID_DEPTH)]


def fused(groups, slabs, residual, capacity):
    steps, thick, second, third = residual.shape
    length, devices = groups * steps, groups * slabs
    planes, extent = thick // groups, slabs * thick
    tile = (second, third)
    ratio_step = ALPHA_CORNER ** (1.0 / length)
    angle = 2.0 * np.pi / length * np.arange(devices)
    table = np.stack(
        [
            (1.0 - ratio_step * np.cos(angle)) / STEP_SIZE,
            ratio_step * np.sin(angle) / STEP_SIZE,
            (1.0 - ratio_step * np.cos(angle)) / STEP_SIZE,
        ],
        axis=1,
    )
    table[0, 1], table[0, 2] = 0.0, (1.0 + ratio_step) / STEP_SIZE
    extents = level_extents(extent)
    vmem = lambda *shape: pltpu.VMEM(shape + tile, jnp.float32)
    sems = lambda *shape: pltpu.SemaphoreType.DMA(shape)
    scratch = [
        vmem(planes, length),
        vmem(planes, devices, 2),
        vmem(planes, devices, 2),
        vmem(planes, length),
        vmem(extent, 2),
        *[vmem(n, 2) for n in extents],
        *[vmem(n) for n in extents],
        *[vmem(n, 3) for n in extents],
        *[vmem(n + 2, 2) for n in extents],
        *[vmem(n + 2, 2) for n in extents],
        sems(planes, groups),
        sems(planes, groups),
        sems(planes),
        sems(planes),
        sems(planes),
        sems(planes),
        sems(planes, groups),
        sems(planes, groups),
        sems(3 * planes + 2),
        sems(slabs),
        sems(slabs),
        pltpu.SemaphoreType.REGULAR((slabs // 2,)),
        pltpu.VMEM(residual.shape, jnp.float32),
    ]
    return pl.pallas_call(
        functools.partial(whole_kernel, groups, slabs, table),
        out_shape=jax.ShapeDtypeStruct(residual.shape, jnp.float32),
        in_specs=[
            pl.BlockSpec(memory_space=pltpu.HBM),
            pl.BlockSpec(memory_space=pltpu.HBM),
        ],
        out_specs=pl.BlockSpec(memory_space=pltpu.VMEM),
        scratch_shapes=scratch,
        compiler_params=pltpu.CompilerParams(
            collective_id=0, has_side_effects=True, vmem_limit_bytes=32 * 2**20
        ),
    )(residual, capacity)


def fits_fused(groups, slabs, residual):
    steps, thick, second, third = residual.shape
    length = groups * steps
    power = length & (length - 1) == 0
    return (
        power
        and groups * slabs == length // 2
        and slabs % 2 == 0
        and thick % groups == 0
        and all(n % 2 == 0 and n % min(n, BLOCK) == 0 for n in level_extents(slabs * thick))
        and (second, third) == (8, 128)
    )


def either(residual, capacity):
    groups, slabs = lax.axis_size("tm"), lax.axis_size("space")
    if fits_fused(groups, slabs, residual):
        return fused(groups, slabs, residual, capacity)
    return on_device(residual, capacity)


def solution(mesh):
    return jax.shard_map(
        either,
        mesh=mesh,
        in_specs=(P("tm", "space", None, None), P("space", None, None)),
        out_specs=P("tm", "space", None, None),
        check_vma=False,
    )
```
